32 devices in a mesh: section: 4 (over y, x), dp: 2 (over core), head: 4 (over z).
Axes of the slice: x: 2, y: 2, z: 4, core: 2. Of those that a mesh axis runs over, the one named last changes fastest.
Arguments:
- queries: bfloat16 [2, 4, 256, 12288], P(None, 'section', 'dp', 'head'), may hold values from -40 to 40
- latents: bfloat16 [2, 4, 256, 576], P(None, 'section', 'dp'), may hold values from -6 to 6
- out_grad: bfloat16 [2, 4, 256, 8192], P(None, 'section', 'dp', 'head'), may hold values from -6 to 6
- segment_ids: int32 [2, 4, 256], P(None, 'section', 'dp'), may hold values from 0 to 7, never falling along the last dimension, each value on 1 to 128 neighbouring positions
- up_weight: bfloat16 [2, 4, 512, 16384], P(None, 'section', None, 'head'), may hold values from -0.25 to 0.25
Outputs:
- query_grad: bfloat16 [2, 4, 256, 12288], P(None, 'section', 'dp', 'head')
- latent_grad: bfloat16 [2, 4, 256, 576], P(None, 'section', ('dp', 'head'))
- weight_grad: float32 [4, 512, 16384], P('section', 'dp', 'head')
The draws below stay inside these ranges and needn't reach their ends.
All inputs are finite; a program needn't handle non-finite values.
Results may differ from the reference program's by a relative error of at most 0.017.
Values may be sent and summed in bfloat16 or wider, within the bound.
A program may use at most 64 MiB of HBM per device.

```python
import math
import jax
import jax.numpy as jnp
import numpy as np
from jax import lax

LATENT = 512
ROPE = 64
NOPE = 128
VDIM = 128
HEADS = 64
TOK = 128
SECTIONS = 4
ROWS = 256
N_DP = 2


def joint_draw(key):
    base = jax.random.fold_in(key, 11)
    first, second = jax.random.split(base, 2)
    query_shape = (2, SECTIONS, ROWS, HEADS, NOPE + ROPE)
    latent_shape = (2, SECTIONS, ROWS, LATENT + ROPE)
    latent_vals = jnp.clip(jax.random.normal(first, latent_shape, jnp.float32), -6.0, 6.0)
    query_vals = jnp.clip(jax.random.normal(second, query_shape, jnp.float32), -6.0, 6.0)
    return (query_vals.reshape(2, SECTIONS, ROWS, HEADS * (NOPE + ROPE)), latent_vals)


def draw_queries(key, part):
    return joint_draw(key)[0].astype(jnp.bfloat16)


def draw_latents(key, part):
    return joint_draw(key)[1].astype(jnp.bfloat16)


def steps_of(own_key, shape, cuts, smallest, high):
    def one(position, shards_of):
        heights = jax.random.uniform(jax.random.fold_in(jax.random.fold_in(own_key, 6), position), (shards_of,), jnp.float32, smallest / len(cuts), high / len(cuts))
        return jnp.repeat(jnp.exp(heights), shape[position] // shards_of).reshape((-1,) + (1,) * (len(shape) - position - 1))

    loudness = one(*cuts[0])
    for cut in cuts[1:]:
        loudness = loudness * one(*cut)
    return loudness


def profile(number_of, total, limit, lean):
    portions = [(1 << 20) // math.isqrt(rank ** lean) + 1 for rank in range(2, number_of + 1)]
    spare, holding = total - limit - (number_of - 1), [1] * (number_of - 1)
    while spare > 0:
        candidates = [i for i in range(number_of - 1) if holding[i] < limit]
        whole, left = sum([portions[i] for i in candidates]), spare
        for i in candidates:
            more = min(limit - holding[i], max(1, left * portions[i] // whole), spare)
            holding[i] = holding[i] + more
            spare = spare - more
    return np.array([limit] + holding)


def uneven(rng, amount, total, bound, skew):
    if amount == 2:
        one = jax.random.randint(rng, (), max(1, total - bound), min(bound, total - 1) + 1)
        return jnp.stack([one, total - one])
    sizes = jnp.asarray(profile(amount, total, bound, skew), jnp.int32)
    twos = (amount - 1) // 2
    donor, receiver = sizes[1:1 + 2 * twos:2], sizes[2:2 + 2 * twos:2]
    slack = jnp.minimum(donor - 1, bound - receiver)
    moved = jax.random.randint(jax.random.fold_in(rng, 1), (twos,), 0, 1 << 20) % (slack + 1)
    sizes = sizes.at[1:1 + 2 * twos:2].set(donor - moved).at[2:2 + 2 * twos:2].set(receiver + moved)
    return sizes[jax.random.permutation(jax.random.fold_in(rng, 2), amount)]


def normal_values(rng, shape, width, reach, cuts=(), held_as=jnp.bfloat16):
    gain = steps_of(rng, shape, cuts, -0.22, 0.18) if cuts else 1.0
    drawn = jax.random.normal(rng, shape, jnp.float32) * width * gain
    return jnp.minimum(jnp.maximum(drawn, -reach), reach).astype(held_as)


def setup_inputs(seed: int = 0) -> dict:
    seeds = jax.random.split(jax.random.key(seed), 6)
    return {
        "queries": draw_queries(jax.random.fold_in(seeds[5], 71), 0),
        "latents": draw_latents(jax.random.fold_in(seeds[5], 71), 0),
        "out_grad": normal_values(seeds[2], (2, SECTIONS, ROWS, HEADS * VDIM), 1.0, 6.0, ((1, 4), (2, 2), (3, 4))),
        "segment_ids": jax.vmap(lambda own: jnp.searchsorted(jnp.cumsum(uneven(own, 4 * N_DP, ROWS, TOK, 1)), jnp.arange(ROWS), side="right"))(jax.random.split(seeds[3], 2 * SECTIONS)).reshape((2, SECTIONS, ROWS)).astype(jnp.int32),
        "up_weight": normal_values(seeds[4], (2, SECTIONS, LATENT, HEADS * (NOPE + VDIM)), LATENT ** -0.5, 0.25, ((1, 4), (3, 4))),
    }


def micro_grads(queries, latents, out_grad, segment_ids, weight):
    tokens = queries.shape[0]
    latent_plain = latents[:, :LATENT]
    key_rope = latents[:, LATENT:].astype(jnp.float32)
    kv_full = jnp.dot(latent_plain, weight, preferred_element_type=jnp.float32).astype(jnp.bfloat16)
    kv_full = kv_full.astype(jnp.float32).reshape(tokens, HEADS, NOPE + VDIM)
    key_plain = kv_full[..., :NOPE]
    values = kv_full[..., NOPE:]
    query_heads = queries.astype(jnp.float32).reshape(tokens, HEADS, NOPE + ROPE)
    query_plain = query_heads[..., :NOPE]
    query_rope = query_heads[..., NOPE:]
    out_heads = out_grad.astype(jnp.float32).reshape(tokens, HEADS, VDIM)
    scale = (NOPE + ROPE) ** -0.5
    scores = (jnp.einsum('thd,shd->hts', query_plain, key_plain) + jnp.einsum('thd,sd->hts', query_rope, key_rope)) * scale
    positions = jnp.arange(tokens)
    allowed = (positions[:, None] >= positions[None, :]) & (segment_ids[:, None] == segment_ids[None, :])
    scores = jnp.where(allowed[None], scores, jnp.float32(-1e30))
    probs = jax.nn.softmax(scores, axis=-1)
    grad_probs = jnp.einsum('thd,shd->hts', out_heads, values)
    delta = jnp.sum(probs * grad_probs, axis=-1, keepdims=True)
    score_grad = (probs * (grad_probs - delta) * scale).astype(jnp.bfloat16).astype(jnp.float32)
    probs_low = probs.astype(jnp.bfloat16).astype(jnp.float32)
    value_grad = jnp.einsum('hts,thd->shd', probs_low, out_heads)
    key_grad = jnp.einsum('hts,thd->shd', score_grad, query_plain)
    rope_grad = jnp.einsum('hts,thd->sd', score_grad, query_rope)
    grad_plain = jnp.einsum('hts,shd->thd', score_grad, key_plain)
    grad_rope = jnp.einsum('hts,sd->thd', score_grad, key_rope)
    query_grad = jnp.concatenate([grad_plain, grad_rope], -1).reshape(tokens, -1).astype(jnp.bfloat16)
    kv_grad = jnp.concatenate([key_grad, value_grad], -1).reshape(tokens, -1).astype(jnp.bfloat16)
    latent_part = jnp.dot(kv_grad, weight.T, preferred_element_type=jnp.float32)
    local_latent = jnp.concatenate([latent_part, rope_grad], 1).astype(jnp.bfloat16)
    partial_value = jnp.dot(latent_plain.T, kv_grad, preferred_element_type=jnp.float32)
    return query_grad, local_latent, partial_value


def direction_grads(queries, latents, out_grad, segment_ids, weights):
    sections = queries.shape[0]
    query_items = queries.reshape(sections, N_DP, TOK, -1)
    latent_items = latents.reshape(sections, N_DP, TOK, -1)
    out_items = out_grad.reshape(sections, N_DP, TOK, -1)
    segment_items = segment_ids.reshape(sections, N_DP, TOK)

    def one_section(items):
        q_section, l_section, o_section, s_section, weight = items

        def step(total, inner):
            query_grad, local_latent, partial_value = micro_grads(inner[0], inner[1], inner[2], inner[3], weight)
            rounded = lax.optimization_barrier(partial_value.astype(jnp.bfloat16)).astype(jnp.float32)
            return total + rounded, (query_grad, local_latent)

        start = jnp.zeros((LATENT, HEADS * (NOPE + VDIM)), jnp.float32)
        total, (query_grads, latent_grads) = lax.scan(step, start, (q_section, l_section, o_section, s_section))
        return query_grads, latent_grads, total

    query_grads, latent_grads, totals = lax.map(one_section, (query_items, latent_items, out_items, segment_items, weights))
    return query_grads.reshape(sections, N_DP * TOK, -1), latent_grads.reshape(sections, N_DP * TOK, -1), totals


def reference(queries, latents, out_grad, segment_ids, up_weight):
    q_fwd, l_fwd, w_fwd = direction_grads(queries[0], latents[0], out_grad[0], segment_ids[0], up_weight[0])
    q_rev, l_rev, w_rev = direction_grads(queries[1], latents[1], out_grad[1], segment_ids[1], up_weight[1])
    q_fwd = jnp.concatenate([q_fwd[1:], jnp.zeros_like(q_fwd[:1])], 0)
    l_fwd = jnp.concatenate([l_fwd[1:], jnp.zeros_like(l_fwd[:1])], 0)
    q_rev = jnp.concatenate([jnp.zeros_like(q_rev[:1]), q_rev[:-1]], 0)
    l_rev = jnp.concatenate([jnp.zeros_like(l_rev[:1]), l_rev[:-1]], 0)
    query_grad = jnp.stack([q_fwd, q_rev], 0)
    latent_grad = jnp.stack([l_fwd, l_rev], 0)
    weight_grad = w_fwd + w_rev[::-1]
    return query_grad, latent_grad, weight_grad
```

```python
import functools

import jax
import jax.numpy as jnp
from jax import lax
from jax.experimental import pallas as pl
from jax.experimental.pallas import tpu as pltpu
from jax.sharding import PartitionSpec as P

ROPE = 64
NOPE = 128
VDIM = 128
QDIM = NOPE + ROPE
KVDIM = NOPE + VDIM


def dot(a, b, contract):
    return lax.dot_general(a, b, ((contract[:1], contract[1:]), ((), ())), preferred_element_type=jnp.float32)


def grads_kernel(
    heads, queries, latents, out_grad, seg_col, seg_row, weight, query_grad, kv_grad, latent_out, acc, rope_acc
):
    step = pl.program_id(0)
    tokens = queries.shape[0]
    latent = weight.shape[0]

    @pl.when(step == 0)
    def _():
        acc[...] = jnp.zeros_like(acc)
        rope_acc[...] = jnp.zeros_like(rope_acc)

    scale = QDIM ** (-0.5)
    rows = lax.broadcasted_iota(jnp.int32, (tokens, tokens), 0)
    columns = lax.broadcasted_iota(jnp.int32, (tokens, tokens), 1)
    allowed = (rows >= columns) & (seg_col[...] == seg_row[...])
    key_rope = latents[:, latent:]
    kv = dot(latents[:, :latent], weight[...], (1, 0)).astype(jnp.bfloat16)
    query_block = queries[...]
    out_block = out_grad[...]
    query_parts, kv_parts = [], []
    rope_sum = rope_acc[...]
    for h in range(heads):
        key = jnp.concatenate([kv[:, h * KVDIM : h * KVDIM + NOPE], key_rope], 1)
        value = kv[:, h * KVDIM + NOPE : (h + 1) * KVDIM]
        query = query_block[:, h * QDIM : (h + 1) * QDIM]
        out = out_block[:, h * VDIM : (h + 1) * VDIM]
        scores = jnp.where(allowed, dot(query, key, (1, 1)) * scale, jnp.float32(-1e30))
        powers = jnp.exp(scores - jnp.max(scores, axis=-1, keepdims=True))
        probs = powers / jnp.sum(powers, axis=-1, keepdims=True)
        grad_probs = dot(out, value, (1, 1))
        delta = jnp.sum(probs * grad_probs, axis=-1, keepdims=True)
        score_grad = (probs * (grad_probs - delta) * scale).astype(jnp.bfloat16)
        value_grad = dot(probs.astype(jnp.bfloat16), out, (0, 0))
        key_grad = dot(score_grad, query, (0, 0))
        rope_sum += key_grad[:, NOPE:]
        query_parts.append(dot(score_grad, key, (1, 0)))
        kv_parts += [key_grad[:, :NOPE].astype(jnp.bfloat16), value_grad.astype(jnp.bfloat16)]
    rope_acc[...] = rope_sum
    query_grad[...] = jnp.concatenate(query_parts, 1).astype(jnp.bfloat16)
    kv_out = jnp.concatenate(kv_parts, 1)
    kv_grad[...] = kv_out
    acc[...] += dot(kv_out, weight[...], (1, 1))

    @pl.when(step == pl.num_programs(0) - 1)
    def _():
        latent_out[...] = jnp.concatenate([acc[...], rope_acc[...]], 1).astype(jnp.bfloat16)


def head_grads(side, queries, latents, out_grad, segment_ids, up_weight):
    tokens = queries.shape[2]
    latent, width = up_weight.shape[2:]
    features = latents.shape[3]
    heads_here = width // KVDIM
    heads = next(k for k in (4, 2, 1) if heads_here % k == 0)
    steps = heads_here // heads
    seg = segment_ids[side, 0]

    def columns_of(size, first):
        return pl.BlockSpec((None, None, first, size), lambda i: (side, 0, 0, i))

    flops = 2 * tokens * width * latent * 2 + 2 * tokens * tokens * heads_here * 5 * KVDIM
    return pl.pallas_call(
        functools.partial(grads_kernel, heads),
        grid=(steps,),
        in_specs=[
            columns_of(heads * QDIM, tokens),
            pl.BlockSpec((None, None, tokens, features), lambda i: (side, 0, 0, 0)),
            columns_of(heads * VDIM, tokens),
            pl.BlockSpec((tokens, 1), lambda i: (0, 0)),
            pl.BlockSpec((1, tokens), lambda i: (0, 0)),
            columns_of(heads * KVDIM, latent),
        ],
        out_specs=[
            pl.BlockSpec((tokens, heads * QDIM), lambda i: (0, i)),
            pl.BlockSpec((tokens, heads * KVDIM), lambda i: (0, i)),
            pl.BlockSpec((tokens, features), lambda i: (0, 0)),
        ],
        out_shape=[
            jax.ShapeDtypeStruct((tokens, heads_here * QDIM), jnp.bfloat16),
            jax.ShapeDtypeStruct((tokens, width), jnp.bfloat16),
            jax.ShapeDtypeStruct((tokens, features), jnp.bfloat16),
        ],
        scratch_shapes=[
            pltpu.VMEM((tokens, latent), jnp.float32),
            pltpu.VMEM((tokens, features - latent), jnp.float32),
        ],
        cost_estimate=pl.CostEstimate(flops=4 * flops, bytes_accessed=8 * latent * width, transcendentals=0),
        name="grads_fwd" if side == 0 else "grads_rev",
    )(queries, latents, out_grad, seg[:, None], seg[None, :], up_weight)


def weight_kernel(pieces, *refs):
    total = None
    for k in range(pieces):
        term = dot(refs[k][...], refs[pieces + k][...], (0, 0))
        total = term if total is None else total + term
    refs[-1][...] = total


def weight_sum(latent_rows, kv_grads):
    pieces = len(kv_grads)
    tokens, width = kv_grads[0].shape
    rows = latent_rows[0].shape[1]
    block = next(b for b in (1024, 512, 256) if width % b == 0)
    return pl.pallas_call(
        functools.partial(weight_kernel, pieces),
        grid=(width // block,),
        in_specs=[pl.BlockSpec((tokens, rows), lambda i: (0, 0))] * pieces
        + [pl.BlockSpec((tokens, block), lambda i: (0, i))] * pieces,
        out_specs=pl.BlockSpec((rows, block), lambda i: (0, i)),
        out_shape=jax.ShapeDtypeStruct((rows, width), jnp.float32),
        cost_estimate=pl.CostEstimate(
            flops=2 * pieces * tokens * rows * width,
            bytes_accessed=2 * pieces * tokens * width + 4 * rows * width,
            transcendentals=0,
        ),
        name="weight_sum",
    )(*latent_rows, *kv_grads)


def turns(block, axis):
    n = lax.axis_size(axis)
    return [block] + [
        lax.ppermute(block, axis, [(i, (i + k) % n) for i in range(n)]) for k in range(1, n)
    ]


def shift(block, axis, distance):
    n = lax.axis_size(axis)
    return lax.ppermute(block, axis, [(i, i + distance) for i in range(n) if 0 <= i + distance < n])


def mirror(block, axis):
    n = lax.axis_size(axis)
    return lax.ppermute(block, axis, [(i, n - 1 - i) for i in range(n)])


def scatter_sum(block, axis):
    n = lax.axis_size(axis)
    me = lax.axis_index(axis)
    rows = block.shape[0] // n

    def piece(k):
        return lax.dynamic_slice_in_dim(block, lax.rem(me + k, n) * rows, rows, 0)

    total = piece(0).astype(jnp.float32)
    for k in range(1, n):
        total += lax.ppermute(piece(k), axis, [(i, (i + k) % n) for i in range(n)]).astype(jnp.float32)
    return total.astype(jnp.bfloat16)


def body(queries, latents, out_grad, segment_ids, up_weight):
    latent = up_weight.shape[2]
    args = (queries, latents, out_grad, segment_ids, up_weight)
    dp = lax.axis_size("dp")
    rows = latent // dp
    first = lax.axis_index("dp") * rows

    plain_fwd = turns(latents[0, 0, :, :latent], "dp")
    plain_rev = turns(mirror(latents[1, 0, :, :latent], "section"), "dp")
    latent_rows = [lax.dynamic_slice_in_dim(x, first, rows, 1) for x in plain_fwd + plain_rev]

    query_rev, kv_rev, local_rev = head_grads(1, *args)
    kv_mirrored = mirror(kv_rev, "section")
    query_rev_in = shift(query_rev, "section", 1)

    query_fwd, kv_fwd, local_fwd = head_grads(0, *args)
    query_fwd_in = shift(query_fwd, "section", -1)
    kv_grads = turns(kv_fwd, "dp") + turns(kv_mirrored, "dp")

    latent_rev_in = shift(scatter_sum(local_rev, "head"), "section", 1)
    latent_fwd_in = shift(scatter_sum(local_fwd, "head"), "section", -1)

    weight_grad = weight_sum(latent_rows, kv_grads)[None]
    query_grad = jnp.stack([query_fwd_in, query_rev_in], 0)[:, None]
    latent_grad = jnp.stack([latent_fwd_in, latent_rev_in], 0)[:, None]
    return (query_grad, latent_grad, weight_grad)


def solution(mesh):
    in_specs = (
        P(None, "section", "dp", "head"),
        P(None, "section", "dp", None),
        P(None, "section", "dp", "head"),
        P(None, "section", "dp"),
        P(None, "section", None, "head"),
    )
    out_specs = (
        P(None, "section", "dp", "head"),
        P(None, "section", ("dp", "head"), None),
        P("section", "dp", "head"),
    )
    return jax.shard_map(body, mesh=mesh, in_specs=in_specs, out_specs=out_specs, check_vma=False)
```

```python
import functools

import jax
import jax.numpy as jnp
from jax import lax
from jax.experimental import pallas as pl
from jax.experimental.pallas import tpu as pltpu
from jax.sharding import PartitionSpec as P

ROPE = 64
NOPE = 128
VDIM = 128
QDIM = NOPE + ROPE
KVDIM = NOPE + VDIM


def dot(a, b, contract):
    return lax.dot_general(a, b, ((contract[:1], contract[1:]), ((), ())), preferred_element_type=jnp.float32)


def grads_kernel(
    heads, side, queries, latents, out_grad, segment_ids, weight, query_grad, kv_grad, latent_out, acc, rope_acc
):
    step = pl.program_id(0)
    tokens = queries.shape[0]
    latent = weight.shape[0]

    @pl.when(step == 0)
    def _():
        kv_grad[:, pl.num_programs(0) * heads * KVDIM :] = latents[:, :latent]
        acc[...] = jnp.zeros_like(acc)
        rope_acc[...] = jnp.zeros_like(rope_acc)

    scale = QDIM ** (-0.5)
    rows = lax.broadcasted_iota(jnp.int32, (tokens, tokens), 0)
    columns = lax.broadcasted_iota(jnp.int32, (tokens, tokens), 1)
    segments = jnp.broadcast_to(segment_ids[side].astype(jnp.float32), (tokens, tokens))
    allowed = (rows >= columns) & (segments == segments.T)
    key_rope = latents[:, latent:]
    kv = dot(latents[:, :latent], weight[...], (1, 0)).astype(jnp.bfloat16)
    query_block = queries[...]
    out_block = out_grad[...]
    query_parts, kv_parts = [], []
    rope_sum = rope_acc[...]
    for h in range(heads):
        key = jnp.concatenate([kv[:, h * KVDIM : h * KVDIM + NOPE], key_rope], 1)
        value = kv[:, h * KVDIM + NOPE : (h + 1) * KVDIM]
        query = query_block[:, h * QDIM : (h + 1) * QDIM]
        out = out_block[:, h * VDIM : (h + 1) * VDIM]
        scores = jnp.where(allowed, dot(query, key, (1, 1)) * scale, jnp.float32(-1e30))
        powers = jnp.exp(scores - jnp.max(scores, axis=-1, keepdims=True))
        probs = powers / jnp.sum(powers, axis=-1, keepdims=True)
        grad_probs = dot(out, value, (1, 1))
        delta = jnp.sum(probs * grad_probs, axis=-1, keepdims=True)
        score_grad = (probs * (grad_probs - delta) * scale).astype(jnp.bfloat16)
        value_grad = dot(probs.astype(jnp.bfloat16), out, (0, 0))
        key_grad = dot(score_grad, query, (0, 0))
        rope_sum += key_grad[:, NOPE:]
        query_parts.append(dot(score_grad, key, (1, 0)))
        kv_parts += [key_grad[:, :NOPE].astype(jnp.bfloat16), value_grad.astype(jnp.bfloat16)]
    rope_acc[...] = rope_sum
    query_grad[...] = jnp.concatenate(query_parts, 1).astype(jnp.bfloat16)
    kv_out = jnp.concatenate(kv_parts, 1)
    block = heads * KVDIM
    kv_grad[:, pl.ds(pl.multiple_of(step * block, block), block)] = kv_out
    acc[...] += dot(kv_out, weight[...], (1, 1))

    @pl.when(step == pl.num_programs(0) - 1)
    def _():
        latent_out[...] = jnp.concatenate([acc[...], rope_acc[...]], 1).astype(jnp.bfloat16)


def head_grads(side, queries, latents, out_grad, segment_ids, up_weight):
    tokens = queries.shape[2]
    latent, width = up_weight.shape[2:]
    features = latents.shape[3]
    heads_here = width // KVDIM
    heads = next(k for k in (4, 2, 1) if heads_here % k == 0)
    steps = heads_here // heads

    def columns_of(size, first):
        return pl.BlockSpec((None, None, first, size), lambda i: (side, 0, 0, i))

    flops = 2 * tokens * width * latent * 2 + 2 * tokens * tokens * heads_here * 5 * KVDIM
    return pl.pallas_call(
        functools.partial(grads_kernel, heads, side),
        grid=(steps,),
        in_specs=[
            columns_of(heads * QDIM, tokens),
            pl.BlockSpec((None, None, tokens, features), lambda i: (side, 0, 0, 0)),
            columns_of(heads * VDIM, tokens),
            pl.BlockSpec(segment_ids.shape, lambda i: (0, 0, 0)),
            columns_of(heads * KVDIM, latent),
        ],
        out_specs=[
            pl.BlockSpec((tokens, heads * QDIM), lambda i: (0, i)),
            pl.BlockSpec((tokens, width + latent), lambda i: (0, 0)),
            pl.BlockSpec((tokens, features), lambda i: (0, 0)),
        ],
        out_shape=[
            jax.ShapeDtypeStruct((tokens, heads_here * QDIM), jnp.bfloat16),
            jax.ShapeDtypeStruct((tokens, width + latent), jnp.bfloat16),
            jax.ShapeDtypeStruct((tokens, features), jnp.bfloat16),
        ],
        scratch_shapes=[
            pltpu.VMEM((tokens, latent), jnp.float32),
            pltpu.VMEM((tokens, features - latent), jnp.float32),
        ],
        cost_estimate=pl.CostEstimate(flops=4 * flops, bytes_accessed=8 * latent * width, transcendentals=0),
        name="grads_fwd" if side == 0 else "grads_rev",
    )(queries, latents, out_grad, segment_ids, up_weight)


def weight_kernel(pieces, *refs):
    total = None
    for k in range(pieces):
        term = dot(refs[0][k], refs[1 + k][...], (0, 0))
        total = term if total is None else total + term
    refs[-1][...] = total


def weight_sum(latent_rows, kv_grads, width):
    pieces = len(kv_grads)
    tokens, rows = latent_rows.shape[1:]
    block = next(b for b in (1024, 512, 256) if width % b == 0)
    return pl.pallas_call(
        functools.partial(weight_kernel, pieces),
        grid=(width // block,),
        in_specs=[pl.BlockSpec((pieces, tokens, rows), lambda i: (0, 0, 0))]
        + [pl.BlockSpec((tokens, block), lambda i: (0, i))] * pieces,
        out_specs=pl.BlockSpec((rows, block), lambda i: (0, i)),
        out_shape=jax.ShapeDtypeStruct((rows, width), jnp.float32),
        cost_estimate=pl.CostEstimate(
            flops=2 * pieces * tokens * rows * width,
            bytes_accessed=2 * pieces * tokens * width + 4 * rows * width,
            transcendentals=0,
        ),
        name="weight_sum",
    )(latent_rows, *kv_grads)


def turns(block, axis):
    n = lax.axis_size(axis)
    return [block] + [
        lax.ppermute(block, axis, [(i, (i + k) % n) for i in range(n)]) for k in range(1, n)
    ]


def shift(block, axis, distance):
    n = lax.axis_size(axis)
    return lax.ppermute(block, axis, [(i, i + distance) for i in range(n) if 0 <= i + distance < n])


def mirror(block, axis):
    n = lax.axis_size(axis)
    return lax.ppermute(block, axis, [(i, n - 1 - i) for i in range(n)])


def body(queries, latents, out_grad, segment_ids, up_weight):
    latent, width = up_weight.shape[2:]
    args = (queries, latents, out_grad, segment_ids, up_weight)
    rows = latent // lax.axis_size("dp")
    first = lax.axis_index("dp") * rows

    query_rev, kv_rev, local_rev = head_grads(1, *args)
    kv_mirrored = mirror(kv_rev, "section")
    query_rev_in = shift(query_rev, "section", 1)

    query_fwd, kv_fwd, local_fwd = head_grads(0, *args)
    query_fwd_in = shift(query_fwd, "section", -1)
    kv_grads = turns(kv_fwd, "dp") + turns(kv_mirrored, "dp")

    local = jnp.stack([local_fwd, local_rev], 0)
    owned = lax.psum_scatter(local, "head", scatter_dimension=1, tiled=True)
    latent_fwd_in = shift(owned[0], "section", -1)
    latent_rev_in = shift(owned[1], "section", 1)

    plain = jnp.stack([x[:, width:] for x in kv_grads], 0)
    latent_rows = lax.dynamic_slice_in_dim(plain, first, rows, 2)
    weight_grad = weight_sum(latent_rows, kv_grads, width)
    weight_grad, query_fwd_in, query_rev_in, latent_fwd_in, latent_rev_in = lax.optimization_barrier(
        (weight_grad, query_fwd_in, query_rev_in, latent_fwd_in, latent_rev_in)
    )
    query_grad = jnp.stack([query_fwd_in, query_rev_in], 0)[:, None]
    latent_grad = jnp.stack([latent_fwd_in, latent_rev_in], 0)[:, None]
    return (query_grad, latent_grad, weight_grad[None])


def solution(mesh):
    in_specs = (
        P(None, "section", "dp", "head"),
        P(None, "section", "dp", None),
        P(None, "section", "dp", "head"),
        P(None, "section", "dp"),
        P(None, "section", None, "head"),
    )
    out_specs = (
        P(None, "section", "dp", "head"),
        P(None, "section", ("dp", "head"), None),
        P("section", "dp", "head"),
    )
    return jax.shard_map(body, mesh=mesh, in_specs=in_specs, out_specs=out_specs, check_vma=False)
```
